32 devices in a mesh: dp: 2 (over x), space: 4 (over y, core), mp: 4 (over z).
Axes of the slice: x: 2, y: 2, z: 4, core: 2. Of those that a mesh axis runs over, the one named last changes fastest.
Arguments:
- teacher_tokens: bfloat16 [16, 4, 16, 16, 1408], P('dp', 'space'), parts along dimension 0, may hold values from -16 to 16
- student_tokens: bfloat16 [16, 4, 16, 16, 1280], P('dp', 'space'), parts along dimension 0, may hold values from -16 to 16
- teacher_head: bfloat16 [2816, 1000], P(('dp', 'space'), 'mp'), parts along dimension 0, may hold values from -1 to 1
- student_head: bfloat16 [2560, 1000], P(('dp', 'space'), 'mp'), parts along dimension 0, may hold values from -1 to 1
- valid: int32 [16, 4, 16, 16], P('dp', 'space'), parts along dimension 0, may hold values from 0 to 1, as said below
Outputs:
- patch_kl: float32 [16, 4, 16, 16], P('dp', 'space'), parts along dimension 0
- image_loss: float32 [16], P('dp'), parts along dimension 0
The draws below stay inside these ranges and needn't reach their ends.
There are 2 independent parts, one for each index of `dp`. The reference program is written for one: setup_inputs(seed, part) draws one part's arguments, and reference() takes and returns one part's arrays. A program takes and returns all parts, laid end to end along the dimension named above; each array names one. Nothing has to cross between parts.
Inputs may be any that keep to these rules, and one draw needn't show every extreme that they name: An image may have no valid patch.
All inputs are finite; a program needn't handle non-finite values.
Results may differ from the reference program's by a relative error of at most 0.0003.
Values may be sent and summed in bfloat16 or wider, within the bound.
A program may use at most 64 MiB of HBM per device.

```python
import math
import jax
import jax.numpy as jnp
from jax import lax

TEACHER_WIDTH = 1408
STUDENT_WIDTH = 1280
CLASSES = 1000
IMAGES = 8
TILE_SIDE = 16
TILES = 4


def head_matrix(key, width, salt):
    values = jax.random.normal(jax.random.fold_in(key, salt), (width, CLASSES), jnp.float32)
    return jnp.clip(values * (3.0 / math.sqrt(width)), -1.0, 1.0)


def token_field(key, width, salt):
    base = jax.random.normal(jax.random.fold_in(key, salt + 1), (IMAGES, TILES, TILE_SIDE, TILE_SIDE, width), jnp.float32)
    base = jnp.clip(base, -6.0, 6.0)
    return base.astype(jnp.bfloat16)


def draw_teacher_tokens(key, part):
    return token_field(key, TEACHER_WIDTH, 100)


def draw_student_tokens(key, part):
    return token_field(key, STUDENT_WIDTH, 200)


def draw_teacher_head(key, part):
    return head_matrix(key, TEACHER_WIDTH, 100).astype(jnp.bfloat16)


def draw_student_head(key, part):
    return head_matrix(key, STUDENT_WIDTH, 200).astype(jnp.bfloat16)


def draw_valid(key, part):
    levels = jax.random.randint(jax.random.fold_in(key, 300), (IMAGES, TILES, TILE_SIDE, TILE_SIDE), 0, 4)
    marks = (levels < 3).astype(jnp.int32)
    image_number = jnp.arange(IMAGES)[:, None, None, None]
    empty = (image_number == IMAGES - 1) & (part % 4 == 3)
    return jnp.where(empty, jnp.zeros_like(marks), marks).astype(jnp.int32)


def setup_inputs(seed: int = 0, part: int = 0) -> dict:
    key_list = jax.random.split(jax.random.key(seed), 6)
    own_keys = jax.random.split(jax.random.fold_in(key_list[5], part), 6)
    return {
        "teacher_tokens": draw_teacher_tokens(jax.random.fold_in(jax.random.fold_in(key_list[5], part), 71), part),
        "student_tokens": draw_student_tokens(jax.random.fold_in(jax.random.fold_in(key_list[5], part), 71), part),
        "teacher_head": draw_teacher_head(jax.random.fold_in(jax.random.fold_in(key_list[5], part), 71), part),
        "student_head": draw_student_head(jax.random.fold_in(jax.random.fold_in(key_list[5], part), 71), part),
        "valid": draw_valid(jax.random.fold_in(jax.random.fold_in(key_list[5], part), 71), part),
    }


def to_grid(x):
    side = math.isqrt(TILES)
    shaped = x.reshape((IMAGES, side, side, TILE_SIDE, TILE_SIDE) + x.shape[4:])
    shaped = jnp.swapaxes(shaped, 2, 3)
    return shaped.reshape((IMAGES, side * TILE_SIDE, side * TILE_SIDE) + x.shape[4:])

def to_tiles(x):
    side = math.isqrt(TILES)
    shaped = x.reshape((IMAGES, side, TILE_SIDE, side, TILE_SIDE) + x.shape[3:])
    shaped = jnp.swapaxes(shaped, 2, 3)
    return shaped.reshape((IMAGES, TILES, TILE_SIDE, TILE_SIDE) + x.shape[3:])

def smooth(logits):
    extent = logits.shape[1]
    padded = jnp.pad(logits, ((0, 0), (1, 1), (1, 1), (0, 0)))
    total = jnp.zeros_like(logits)
    for shift_y in range(3):
        for shift_x in range(3):
            total = total + padded[:, shift_y:shift_y + extent, shift_x:shift_x + extent, :]
    ones = jnp.pad(jnp.ones((extent,), jnp.float32), 1)
    line = ones[:-2] + ones[1:-1] + ones[2:]
    count = line[:, None] * line[None, :]
    return total / count[None, :, :, None]

def reference(teacher_tokens, student_tokens, teacher_head, student_head, valid):
    teacher_grid = to_grid(teacher_tokens)
    student_grid = to_grid(student_tokens)
    extent = teacher_grid.shape[1]
    teacher_logits = jnp.dot(teacher_grid.reshape(-1, TEACHER_WIDTH), teacher_head, preferred_element_type=jnp.float32)
    student_logits = jnp.dot(student_grid.reshape(-1, STUDENT_WIDTH), student_head, preferred_element_type=jnp.float32)
    teacher_logits = teacher_logits.reshape(IMAGES, extent, extent, CLASSES)
    student_logits = student_logits.reshape(IMAGES, extent, extent, CLASSES)
    smoothed = smooth(teacher_logits)
    teacher_logp = jax.nn.log_softmax(smoothed, axis=-1)
    student_logp = jax.nn.log_softmax(student_logits, axis=-1)
    divergence = lax.optimization_barrier(jnp.sum(jnp.exp(teacher_logp) * (teacher_logp - student_logp), axis=-1))
    weights = to_grid(valid).astype(jnp.float32)
    totals = lax.optimization_barrier(jnp.sum(divergence * weights, axis=(1, 2)))
    counts = lax.optimization_barrier(jnp.sum(weights, axis=(1, 2)))
    image_loss = totals / jnp.maximum(counts, 1.0)
    return (to_tiles(divergence), image_loss)
```

```python
import functools
import math

import jax
import jax.numpy as jnp
from jax import lax
from jax.experimental import pallas as pl
from jax.experimental.pallas import tpu as pltpu
from jax.sharding import PartitionSpec as P

MESH = pl.DeviceIdType.MESH
F32 = jnp.float32
BF16 = jnp.bfloat16


def kernel(
    edge, mp, parts_w,
    tt_hbm, ts_hbm, wt_hbm, ws_hbm, valid_hbm,
    kl_hbm, loss_hbm,
    tt, ts, wt, ws, hi, lo, sl, smat, rowbuf, colbuf, corbuf, corh, stats, gath, tot, gtot, wide,
    valid_ref, kl_ref, loss_ref, log_student,
    loc_sem, wsend, wrecv, hsend, hrecv, ssend, srecv, tsend, trecv, known,
):
    t = lax.axis_index("space")
    m = lax.axis_index("mp")
    row, col = t // 2, t % 2
    across = 1 - col + 2 * row
    below = col + 2 * (1 - row)
    diag = 3 - t
    images = tt.shape[0]
    area = edge * edge

    barrier = pltpu.get_barrier_semaphore()
    for peer in (across, below, diag):
        pl.semaphore_signal(barrier, inc=1, device_id={"space": peer}, device_id_type=MESH)
    has_left, has_right = m > 0, m < mp - 1

    @pl.when(has_left)
    def _():
        pl.semaphore_signal(barrier, inc=1, device_id={"mp": m - 1}, device_id_type=MESH)

    @pl.when(has_right)
    def _():
        pl.semaphore_signal(barrier, inc=1, device_id={"mp": m + 1}, device_id_type=MESH)

    local = []
    for k, (src, w) in enumerate(((wt_hbm, wt), (ws_hbm, ws))):
        n = src.shape[0]
        dst = w.at[pl.ds(pl.multiple_of(t * n, 16), n)]
        local.append(pltpu.make_async_copy(src, dst, loc_sem.at[k]))
    local.append(pltpu.make_async_copy(tt_hbm, tt, loc_sem.at[2]))
    local.append(pltpu.make_async_copy(ts_hbm, ts, loc_sem.at[3]))
    local.append(pltpu.make_async_copy(valid_hbm, valid_ref, loc_sem.at[4]))
    for c in local:
        c.start()

    local[0].wait()
    pl.semaphore_wait(barrier, 3 + has_left.astype(jnp.int32) + has_right.astype(jnp.int32))

    def piece(w, owner, chunk):
        n = w.shape[0] // 4
        size = n // parts_w
        return w.at[pl.ds(pl.multiple_of(owner * n + chunk * size, 16), size)]

    def move(w, k, kind, owner, chunk, peer):
        i = (k * 3 + kind) * parts_w + chunk
        ref = piece(w, owner, chunk)
        return pltpu.make_async_remote_copy(
            src_ref=ref, dst_ref=ref, send_sem=wsend.at[i], recv_sem=wrecv.at[i],
            device_id={"space": peer}, device_id_type=MESH,
        )

    moves = {}
    for k, w in enumerate((wt, ws)):
        for chunk in range(parts_w):
            moves[k, 0, chunk] = move(w, k, 0, t, chunk, below)
            moves[k, 1, chunk] = move(w, k, 1, t, chunk, across)
            moves[k, 2, chunk] = move(w, k, 2, below, chunk, across)
    for k in range(2):
        if k == 1:
            local[1].wait()
        for chunk in range(parts_w):
            moves[k, 0, chunk].start()
            moves[k, 1, chunk].start()

    def present(k, side, step):
        @pl.when((m + step >= 0) & (m + step < mp) & (m - k * step >= 0) & (m - k * step < mp))
        def _():
            pl.semaphore_signal(known.at[side, k - 1], inc=1, device_id={"mp": m + step}, device_id_type=MESH)

    def heard(k, side, step):
        @pl.when((m - step >= 0) & (m - step < mp) & (m - (k + 1) * step >= 0) & (m - (k + 1) * step < mp))
        def _():
            pl.semaphore_wait(known.at[side, k - 1], 1)

    if mp > 2:
        for side, step in enumerate((1, -1)):
            present(1, side, step)

    p_y = lax.broadcasted_iota(jnp.int32, (edge, edge, area + 2 * edge), 0).reshape(area, area + 2 * edge)
    p_x = lax.broadcasted_iota(jnp.int32, (edge, edge, area + 2 * edge), 1).reshape(area, area + 2 * edge)
    q = lax.broadcasted_iota(jnp.int32, (area, area + 2 * edge), 1)
    e_y = (edge - 1) * (1 - row)
    e_x = (edge - 1) * (1 - col)
    h_y = edge * (1 - row) - row
    h_x = edge * (1 - col) - col
    in_row = (q >= area) & (q < area + edge)
    in_col = q >= area + edge
    q_y = jnp.where(in_row, h_y, jnp.where(in_col, q - area - edge, q // edge))
    q_x = jnp.where(in_row, q - area, jnp.where(in_col, h_x, q % edge))
    near = (jnp.abs(p_y - q_y) <= 1) & (jnp.abs(p_x - q_x) <= 1)
    smat[...] = jnp.where(near, 1.0, 0.0).astype(BF16)

    local[4].wait()
    for r in range(edge):
        wide[:, r * edge : (r + 1) * edge] = valid_ref[:, r, :].astype(F32)

    def arrive(k, w):
        for chunk in range(parts_w):
            move(w, k, 0, below, chunk, below).wait_recv()
            moves[k, 2, chunk].start()
        for chunk in range(parts_w):
            move(w, k, 1, across, chunk, across).wait_recv()
            move(w, k, 2, diag, chunk, across).wait_recv()

    arrive(0, wt)
    local[2].wait()
    edge_tokens = tt[:, pl.ds(pl.multiple_of(e_y * edge, 16), edge), :].reshape(images * edge, tt.shape[-1])
    edge_row = jnp.dot(edge_tokens, wt[...], preferred_element_type=F32).reshape(images, edge, -1)
    rowbuf[...] = edge_row.astype(BF16)
    corbuf[...] = jnp.where(col == 0, edge_row[:, edge - 1, :], edge_row[:, 0, :])
    row_move = pltpu.make_async_remote_copy(
        src_ref=rowbuf, dst_ref=hi.at[:, pl.ds(area, edge), :], send_sem=hsend.at[0], recv_sem=hrecv.at[0],
        device_id={"space": below}, device_id_type=MESH,
    )
    cor_move = pltpu.make_async_remote_copy(
        src_ref=corbuf, dst_ref=corh, send_sem=hsend.at[1], recv_sem=hrecv.at[1],
        device_id={"space": diag}, device_id_type=MESH,
    )
    row_move.start()
    cor_move.start()

    def teacher_dot(i, carry):
        x = jnp.dot(tt[i], wt[...], preferred_element_type=F32)
        top = x.astype(BF16)
        hi[i, pl.ds(0, area), :] = top
        lo[i] = (x - top.astype(F32)).astype(BF16)
        x3 = x.reshape(edge, edge, x.shape[-1])
        side_x = jnp.where(col == 0, x3[:, edge - 1, :], x3[:, 0, :])
        colbuf[i] = side_x.astype(BF16)
        return carry

    lax.fori_loop(0, images, teacher_dot, 0, unroll=8)
    col_move = pltpu.make_async_remote_copy(
        src_ref=colbuf, dst_ref=hi.at[:, pl.ds(area + edge, edge), :], send_sem=hsend.at[2], recv_sem=hrecv.at[2],
        device_id={"space": across}, device_id_type=MESH,
    )
    col_move.start()

    arrive(1, ws)
    local[3].wait()
    for k in range(1, mp - 1):
        for side, step in enumerate((1, -1)):
            heard(k, side, step)
            if k < mp - 2:
                present(k + 1, side, step)

    def student_dot(i, carry):
        student = jnp.dot(ts[i], ws[...], preferred_element_type=F32)
        sl[i] = student
        top_s = jnp.max(student, axis=-1, keepdims=True)
        sum_s = jnp.sum(jnp.exp(student - top_s), axis=-1, keepdims=True)
        log_student[i] = top_s + jnp.log(sum_s)
        return carry

    lax.fori_loop(0, images, student_dot, 0, unroll=8)

    y = lax.broadcasted_iota(jnp.int32, (edge, edge, 1), 0).reshape(area, 1)
    x = lax.broadcasted_iota(jnp.int32, (edge, edge, 1), 1).reshape(area, 1)
    last = 2 * edge - 1
    g_y, g_x = y + row * edge, x + col * edge
    line_y = 1.0 + jnp.where(g_y > 0, 1.0, 0.0) + jnp.where(g_y < last, 1.0, 0.0)
    line_x = 1.0 + jnp.where(g_x > 0, 1.0, 0.0) + jnp.where(g_x < last, 1.0, 0.0)
    inverse = 1.0 / (line_y * line_x)
    at_corner = (y == e_y) & (x == e_x)

    row_move.wait_recv()
    cor_move.wait_recv()
    col_move.wait_recv()

    lane = lax.broadcasted_iota(jnp.int32, (area, 128), 1)

    def image_stats(i, carry):
        total = jnp.dot(smat[...], hi[i], preferred_element_type=F32)
        total += jnp.dot(smat[:, :area], lo[i], preferred_element_type=F32)
        total += jnp.where(at_corner, corh[pl.ds(i, 1), :], 0.0)
        smooth = total * inverse
        student = sl[i]
        top_t = jnp.max(smooth, axis=-1, keepdims=True)
        expo = jnp.exp(smooth - top_t)
        sum_t = jnp.sum(expo, axis=-1, keepdims=True)
        mean = jnp.sum(expo * (smooth - student), axis=-1, keepdims=True) / sum_t
        log_t = top_t + jnp.log(sum_t)
        log_s = log_student[i]
        packed = jnp.where(lane == 0, log_t, jnp.where(lane == 1, mean, log_s))
        turned = packed.T
        for k in range(3):
            stats[k, pl.ds(i, 1), :] = turned[k : k + 1, :]
        return carry

    lax.fori_loop(0, images, image_stats, 0, unroll=4)

    sends = []
    for d in range(1, mp):
        c = pltpu.make_async_remote_copy(
            src_ref=stats, dst_ref=gath.at[d - 1], send_sem=ssend.at[d - 1], recv_sem=srecv.at[d - 1],
            device_id={"mp": lax.rem(m + d, mp)}, device_id_type=MESH,
        )
        c.start()
        sends.append(c)
    for c in sends:
        c.wait_recv()
    logs_t = [stats[0]] + [gath[d, 0] for d in range(mp - 1)]
    means = [stats[1]] + [gath[d, 1] for d in range(mp - 1)]
    logs_s = [stats[2]] + [gath[d, 2] for d in range(mp - 1)]
    top_t = functools.reduce(jnp.maximum, logs_t)
    top_s = functools.reduce(jnp.maximum, logs_s)
    shares = [jnp.exp(v - top_t) for v in logs_t]
    sum_t = sum(shares)
    sum_s = sum(jnp.exp(v - top_s) for v in logs_s)
    weighted = sum(a * b for a, b in zip(shares, means))
    kl = weighted / sum_t - top_t - jnp.log(sum_t) + top_s + jnp.log(sum_s)
    weights = wide[...]
    total = jnp.sum(kl * weights, axis=-1, keepdims=True)
    number = jnp.sum(weights, axis=-1, keepdims=True)
    lanes = lax.broadcasted_iota(jnp.int32, (images, 128), 1)
    tot[...] = jnp.where(lanes == 0, total, number)
    shares_out = []
    for k, peer in enumerate((across, below, diag)):
        c = pltpu.make_async_remote_copy(
            src_ref=tot, dst_ref=gtot.at[k], send_sem=tsend.at[k], recv_sem=trecv.at[k],
            device_id={"space": peer}, device_id_type=MESH,
        )
        c.start()
        shares_out.append(c)
    for r in range(edge):
        kl_ref[:, r, :] = kl[:, r * edge : (r + 1) * edge]
    kl_out = pltpu.make_async_copy(kl_ref, kl_hbm, loc_sem.at[5])
    kl_out.start()
    for c in sends + [row_move, cor_move, col_move] + list(moves.values()):
        c.wait_send()
    for c in shares_out:
        c.wait_recv()
    everything = tot[...] + gtot[0] + gtot[1] + gtot[2]
    loss = everything[:, 0:1] / jnp.maximum(everything[:, 1:2], 1.0)
    loss_ref[...] = jnp.broadcast_to(loss, (images, 128)).T[0:1, :]
    loss_out = pltpu.make_async_copy(loss_ref, loss_hbm, loc_sem.at[6])
    loss_out.start()
    for c in shares_out:
        c.wait_send()
    kl_out.wait()
    loss_out.wait()


def finish(kl_in, loss_in, kl_out, loss_out):
    kl_out[...] = kl_in[...]
    loss_out[...] = loss_in[...]


def fused(teacher_tokens, student_tokens, teacher_head, student_head, valid):
    images, _, edge, _, width = teacher_tokens.shape
    swidth = student_tokens.shape[-1]
    area = edge * edge
    classes = teacher_head.shape[1]
    mp = lax.axis_size("mp")
    parts_w = 2 if teacher_head.shape[0] % 32 == 0 and student_head.shape[0] % 32 == 0 else 1
    anywhere = pl.BlockSpec(memory_space=pl.ANY)
    dma = pltpu.SemaphoreType.DMA
    kl, loss = pl.pallas_call(
        functools.partial(kernel, edge, mp, parts_w),
        out_shape=(
            jax.ShapeDtypeStruct((images, edge, edge), F32),
            jax.ShapeDtypeStruct((1, images), F32),
        ),
        in_specs=[anywhere] * 5,
        out_specs=(anywhere, anywhere),
        scratch_shapes=[
            pltpu.VMEM((images, area, width), BF16),
            pltpu.VMEM((images, area, swidth), BF16),
            pltpu.VMEM((width, classes), BF16),
            pltpu.VMEM((swidth, classes), BF16),
            pltpu.VMEM((images, area + 2 * edge, classes), BF16),
            pltpu.VMEM((images, area, classes), BF16),
            pltpu.VMEM((images, area, classes), F32),
            pltpu.VMEM((area, area + 2 * edge), BF16),
            pltpu.VMEM((images, edge, classes), BF16),
            pltpu.VMEM((images, edge, classes), BF16),
            pltpu.VMEM((images, classes), F32),
            pltpu.VMEM((images, classes), F32),
            pltpu.VMEM((3, images, area), F32),
            pltpu.VMEM((mp - 1, 3, images, area), F32),
            pltpu.VMEM((images, 128), F32),
            pltpu.VMEM((3, images, 128), F32),
            pltpu.VMEM((images, area), F32),
            pltpu.VMEM((images, edge, edge), jnp.int32),
            pltpu.VMEM((images, edge, edge), F32),
            pltpu.VMEM((1, images), F32),
            pltpu.VMEM((images, area, 1), F32),
            dma((7,)),
            dma((6 * parts_w,)),
            dma((6 * parts_w,)),
            dma((3,)),
            dma((3,)),
            dma((mp - 1,)),
            dma((mp - 1,)),
            dma((3,)),
            dma((3,)),
            pltpu.SemaphoreType.REGULAR((2, max(mp - 2, 1))),
        ],
        compiler_params=pltpu.CompilerParams(collective_id=0, has_side_effects=True),
    )(
        teacher_tokens.reshape(images, area, width),
        student_tokens.reshape(images, area, swidth),
        teacher_head,
        student_head,
        valid.reshape(images, edge, edge),
    )
    whole = pl.BlockSpec(memory_space=pltpu.VMEM)
    kl, loss = pl.pallas_call(
        finish,
        out_shape=(jax.ShapeDtypeStruct(kl.shape, F32), jax.ShapeDtypeStruct(loss.shape, F32)),
        in_specs=[whole, whole],
        out_specs=(whole, whole),
    )(kl, loss)
    return kl.reshape(images, 1, edge, edge), loss.reshape(images)


def shifted(block, axis, distance):
    devices = range(lax.axis_size(axis))
    route = [(i - distance, i) for i in devices if i - distance in devices]
    return lax.ppermute(block, axis, route)


def logit_move(values, offset):
    return shifted(values, "space", offset)


def extend(values, mover, side, column):
    left = mover(values[:, :, -1:, :], 1)
    left = jnp.where(column > 0, left, jnp.zeros_like(left))
    right = mover(values[:, :, :1, :], -1)
    right = jnp.where(column < side - 1, right, jnp.zeros_like(right))
    wide = jnp.concatenate([left, values, right], axis=2)
    upper = mover(wide[:, -1:, :, :], side)
    lower = mover(wide[:, :1, :, :], -side)
    return jnp.concatenate([upper, wide, lower], axis=1)


def body(teacher_tokens, student_tokens, teacher_head, student_head, valid):
    side = math.isqrt(lax.axis_size("space"))
    tile_index = lax.axis_index("space")
    tile_row = tile_index // side
    tile_column = tile_index % side
    teacher_tile = teacher_tokens[:, 0]
    student_tile = student_tokens[:, 0]
    images, edge = (teacher_tile.shape[0], teacher_tile.shape[1])
    classes_here = teacher_head.shape[1]
    source_flat = teacher_tile.reshape(-1, teacher_tile.shape[-1])
    student_flat = student_tile.reshape(-1, student_tile.shape[-1])
    teacher_logits = jnp.dot(
        source_flat,
        lax.all_gather(teacher_head, "space", axis=0, tiled=True),
        preferred_element_type=jnp.float32,
    )
    student_logits = jnp.dot(
        student_flat,
        lax.all_gather(student_head, "space", axis=0, tiled=True),
        preferred_element_type=jnp.float32,
    )
    teacher_wide = extend(
        teacher_logits.reshape(images, edge, edge, classes_here), logit_move, side, tile_column
    )
    extent = side * edge
    total = jnp.zeros((images, edge, edge, classes_here), jnp.float32)
    for shift_y in range(3):
        for shift_x in range(3):
            total = total + teacher_wide[:, shift_y : shift_y + edge, shift_x : shift_x + edge, :]
    places_y = tile_row * edge + jnp.arange(edge)
    places_x = tile_column * edge + jnp.arange(edge)
    line_y = 1.0 + (places_y > 0).astype(jnp.float32) + (places_y < extent - 1).astype(jnp.float32)
    line_x = 1.0 + (places_x > 0).astype(jnp.float32) + (places_x < extent - 1).astype(jnp.float32)
    counts = line_y[:, None] * line_x[None, :]
    smoothed = total / counts[None, :, :, None]
    student = student_logits.reshape(images, edge, edge, classes_here)
    top_t, top_s = lax.pmax((jnp.max(smoothed, axis=-1), jnp.max(student, axis=-1)), "mp")
    expo_t = jnp.exp(smoothed - top_t[..., None])
    sum_t, weighted, sum_s = lax.psum(
        (
            jnp.sum(expo_t, axis=-1),
            jnp.sum(expo_t * (smoothed - student), axis=-1),
            jnp.sum(jnp.exp(student - top_s[..., None]), axis=-1),
        ),
        "mp",
    )
    divergence = weighted / sum_t - top_t - jnp.log(sum_t) + top_s + jnp.log(sum_s)
    weights = valid[:, 0].astype(jnp.float32)
    totals, numbers = lax.psum(
        (jnp.sum(divergence * weights, axis=(1, 2)), jnp.sum(weights, axis=(1, 2))), "space"
    )
    image_loss = totals / jnp.maximum(numbers, 1.0)
    return (divergence[:, None], image_loss)


def chosen(teacher_tokens, student_tokens, teacher_head, student_head, valid):
    operands = (teacher_tokens, student_tokens, teacher_head, student_head, valid)
    aligned = (
        lax.axis_size("space") == 4
        and lax.axis_size("mp") > 1
        and teacher_tokens.shape[2] % 16 == 0
        and teacher_head.shape[0] % 16 == 0
        and student_head.shape[0] % 16 == 0
        and teacher_tokens.shape[0] % 8 == 0
    )
    return fused(*operands) if aligned else body(*operands)


def solution(mesh):
    in_specs = (
        P("dp", "space", None, None, None),
        P("dp", "space", None, None, None),
        P(("dp", "space"), "mp"),
        P(("dp", "space"), "mp"),
        P("dp", "space", None, None),
    )
    out_specs = (P("dp", "space", None, None), P("dp"))
    return jax.shard_map(chosen, mesh=mesh, in_specs=in_specs, out_specs=out_specs, check_vma=False)
```

```python
import functools
import math

import jax
import jax.numpy as jnp
from jax import lax
from jax.experimental import pallas as pl
from jax.experimental.pallas import tpu as pltpu
from jax.sharding import PartitionSpec as P

MESH = pl.DeviceIdType.MESH
F32 = jnp.float32
BF16 = jnp.bfloat16


def kernel(
    edge, mp,
    tt_hbm, ts_hbm, wt_hbm, ws_hbm, valid_hbm,
    kl_ref, loss_ref,
    tt, ts, wt, ws, tt_w, ts_w, pre, sl, ex, ec, smat, scol, srow, slift, spick, hal, row_out, col_hl, tok_out, tok_x,
    stat_s, stat_t, gath_s, gath_t, tot, gtot, wide, kl_buf,
    valid_ref,
    loc_sem, wsend, wrecv, hsend, hrecv, ssend, srecv, tsend, trecv,
):
    t = lax.axis_index("space")
    m = lax.axis_index("mp")
    row, col = t // 2, t % 2
    across = 1 - col + 2 * row
    below = col + 2 * (1 - row)
    diag = 3 - t
    images = tt.shape[0]
    area = edge * edge
    groups = stat_t.shape[0]
    per = images // groups
    n_edge = images * edge

    barrier = pltpu.get_barrier_semaphore()
    for peer in (across, below, diag):
        pl.semaphore_signal(barrier, inc=1, device_id={"space": peer}, device_id_type=MESH)
    for d in range(1, mp):
        pl.semaphore_signal(barrier, inc=1, device_id={"mp": lax.rem(m + d, mp)}, device_id_type=MESH)

    local = []
    for k, (src, w) in enumerate(((wt_hbm, wt), (ws_hbm, ws))):
        n = src.shape[0]
        dst = w.at[pl.ds(pl.multiple_of(t * n, 16), n)]
        local.append(pltpu.make_async_copy(src, dst, loc_sem.at[k]))
    local.append(pltpu.make_async_copy(tt_hbm, tt, loc_sem.at[2]))
    local.append(pltpu.make_async_copy(ts_hbm, ts, loc_sem.at[3]))
    local.append(pltpu.make_async_copy(valid_hbm, valid_ref, loc_sem.at[4]))
    for c in local:
        c.start()

    local[0].wait()
    pl.semaphore_wait(barrier, 3 + mp - 1)

    def piece(w, owner, chunk):
        n = w.shape[0] // 4
        large = split(n)
        side = lax.rem(owner, 2)
        if chunk == 0:
            start, size = owner * n + side * (n - large), large
        else:
            start, size = owner * n + (1 - side) * large, n - large
        return w.at[pl.ds(pl.multiple_of(start, 16), size)]

    def move(w, k, kind, owner, chunk, peer):
        i = (k * 3 + kind) * 2 + chunk
        ref = piece(w, owner, chunk)
        return pltpu.make_async_remote_copy(
            src_ref=ref, dst_ref=ref, send_sem=wsend.at[i], recv_sem=wrecv.at[i],
            device_id={"space": peer}, device_id_type=MESH,
        )

    moves = {}
    for k, w in enumerate((wt, ws)):
        for chunk in range(2):
            moves[k, 0, chunk] = move(w, k, 0, t, chunk, below)
            moves[k, 1, chunk] = move(w, k, 1, t, chunk, across)
            moves[k, 2, chunk] = move(w, k, 2, below, chunk, across)
    for k in range(2):
        if k == 1:
            local[1].wait()
        for chunk in range(2):
            if k == 0:
                moves[k, 0, chunk].start()
            moves[k, 1, chunk].start()

    e_y = (edge - 1) * (1 - row)
    e_x = (edge - 1) * (1 - col)

    def one_hot(where):
        return jnp.where(where, 1.0, 0.0).astype(BF16)

    def iota(shape, axis):
        return lax.broadcasted_iota(jnp.int32, shape, axis)

    half = area // 2
    una, aff = pl.multiple_of(row * half, 128), pl.multiple_of((1 - row) * half, 128)
    q, p = iota((area, area), 0), iota((area, area), 1)
    smat[...] = one_hot((jnp.abs(p // edge - q // edge) <= 1) & (jnp.abs(p % edge - q % edge) <= 1))
    h, p = iota((n_edge, area), 0), iota((n_edge, area), 1)
    from_col = (p % edge == e_x) & (jnp.abs(p // edge - h % edge) <= 1)
    h2, p2 = iota((n_edge, half), 0), iota((n_edge, half), 1) + aff
    from_row = (p2 // edge == e_y) & (p2 % edge == h2 % edge)
    for i in range(images):
        scol[i, 0:n_edge, :] = one_hot(from_col & (h // edge == i))
        scol[i, n_edge:, :] = scol[i, 0:n_edge, :]
        srow[i] = one_hot(from_row & (h2 // edge == i))
    a, b = iota((n_edge, n_edge), 0), iota((n_edge, n_edge), 1)
    slift[0:n_edge, :] = one_hot((a // edge == b // edge) & (jnp.abs(a - b) <= 1))
    slift[n_edge:, :] = one_hot((a == b // edge * edge + e_y) & (b % edge == e_x))
    a, b = iota((edge, area), 0), iota((edge, area), 1)
    spick[...] = one_hot(b == a * edge + e_x)
    p = iota((1, area), 1)
    last = 2 * edge - 1
    g_y, g_x = p // edge + row * edge, p % edge + col * edge
    line_y = 1.0 + jnp.where(g_y > 0, 1.0, 0.0) + jnp.where(g_y < last, 1.0, 0.0)
    line_x = 1.0 + jnp.where(g_x > 0, 1.0, 0.0) + jnp.where(g_x < last, 1.0, 0.0)
    inverse = 1.0 / (line_y * line_x)

    def nn(x, y):
        return jnp.dot(x, y, preferred_element_type=F32)

    local[2].wait()
    for i in range(images):
        tok_out[i * edge : (i + 1) * edge, :] = nn(spick[...], tt[i]).astype(BF16)
    tok_move = pltpu.make_async_remote_copy(
        src_ref=tok_out, dst_ref=tok_x.at[pl.ds(n_edge, n_edge)], send_sem=hsend.at[1], recv_sem=hrecv.at[1],
        device_id={"space": across}, device_id_type=MESH,
    )
    tok_move.start()
    tok_x[0:n_edge, :] = tt[:, pl.ds(pl.multiple_of(e_y * edge, 16), edge), :].reshape(n_edge, tt.shape[-1])

    local[4].wait()
    for r in range(edge):
        wide[:, r * edge : (r + 1) * edge] = valid_ref[:, r, :].astype(F32)

    def turn(w, w_t, start, size):
        for j in range(0, size, 128):
            at = pl.multiple_of(start + j, 128)
            w_t[:, pl.ds(at, 128)] = w[pl.ds(at, 128), :].T

    def times(w_t, tokens, start, size):
        at = pl.ds(pl.multiple_of(start, 128), size)
        return lax.dot_general(
            w_t[:, at], tokens[:, at], (((1,), (1,)), ((), ())), preferred_element_type=F32
        )

    def own(k, w):
        for chunk in range(2):
            move(w, k, 1, across, chunk, across).wait_recv()

    def arrive(k, w, chunk):
        move(w, k, 0, below, chunk, below).wait_recv()
        moves[k, 2, chunk].start()

    def arrive_far(k, w, chunk):
        move(w, k, 2, diag, chunk, across).wait_recv()

    def each(f):
        lax.fori_loop(0, images, f, 0, unroll=images)

    class Parts:
        def __init__(self, k):
            large = split(k // 4)
            near = k // 256 * 128
            first, second, far = middle(k)
            self.near = near
            self.outer, self.inner = first, second - first
            self.near_at = row * (k - near)
            self.one_at = (1 - row) * (k - far)
            self.two_at = row * second + (1 - row) * (k - first)
            self.mid_at = row * first + (1 - row) * (k - second)

    of_t, of_s = Parts(tt.shape[-1]), Parts(ts.shape[-1])
    own(0, wt)
    turn(wt, tt_w, of_t.near_at, of_t.near)

    def teacher_near(i, carry):
        pre[i] = times(tt_w, tt.at[i], of_t.near_at, of_t.near)
        return carry

    each(teacher_near)
    own(1, ws)
    turn(ws, ts_w, of_s.near_at, of_s.near)
    local[3].wait()

    def student_near(i, carry):
        sl[i] = times(ts_w, ts.at[i], of_s.near_at, of_s.near)
        return carry

    each(student_near)
    for chunk in range(2):
        moves[0, 0, chunk].wait_send()
    for chunk in range(2):
        moves[1, 0, chunk].start()
    tok_move.wait_recv()
    ec[...] = times(tt_w, tok_x, of_t.near_at, of_t.near)

    arrive(0, wt, 0)
    arrive(0, wt, 1)
    arrive_far(0, wt, 0)
    turn(wt, tt_w, of_t.one_at, of_t.outer)
    turn(wt, tt_w, of_t.two_at, of_t.outer)
    ec[...] += times(tt_w, tok_x, of_t.one_at, of_t.outer) + times(tt_w, tok_x, of_t.two_at, of_t.outer)

    def teacher_outer(i, carry):
        pre[i] += times(tt_w, tt.at[i], of_t.one_at, of_t.outer) + times(tt_w, tt.at[i], of_t.two_at, of_t.outer)
        return carry

    each(teacher_outer)
    arrive_far(0, wt, 1)
    turn(wt, tt_w, of_t.mid_at, of_t.inner)

    def two(x):
        top = x.astype(BF16)
        return top, (x - top.astype(F32)).astype(BF16)

    e_hi, e_lo = two(ec[...] + times(tt_w, tok_x, of_t.mid_at, of_t.inner))
    row_out[...] = (nn(e_hi, slift[...]) + nn(e_lo, slift[...])).astype(BF16)
    row_move = pltpu.make_async_remote_copy(
        src_ref=row_out, dst_ref=hal, send_sem=hsend.at[0], recv_sem=hrecv.at[0],
        device_id={"space": below}, device_id_type=MESH,
    )
    col_hl[:, 0:n_edge] = e_hi[:, n_edge:]
    col_hl[:, n_edge:] = e_lo[:, n_edge:]

    def teacher_inner(i, carry):
        top, rest = two(pre[i] + times(tt_w, tt.at[i], of_t.mid_at, of_t.inner))
        pre[i] = (nn(top, smat[...]) + nn(rest, smat[...]) + nn(col_hl[...], scol[i])) * inverse
        return carry

    each(teacher_inner)

    for chunk in range(2):
        moves[1, 0, chunk].wait_send()
    row_move.start()

    def teacher_half(i, carry):
        top = jnp.max(pre[i, :, pl.ds(una, half)], axis=0, keepdims=True)
        expo = jnp.exp(pre[i, :, pl.ds(una, half)] - top)
        ex[i] = expo
        total = jnp.sum(expo, axis=0, keepdims=True)
        stat_t[i // per, pl.ds(i % per, 1), pl.ds(una, half)] = top + jnp.log(total)
        stat_t[i // per, pl.ds(per + i % per, 1), pl.ds(una, half)] = 1.0 / total
        return carry

    for i in range(images):
        teacher_half(i, 0)

    arrive(1, ws, 0)
    arrive(1, ws, 1)
    arrive_far(1, ws, 0)
    turn(ws, ts_w, of_s.one_at, of_s.outer)
    turn(ws, ts_w, of_s.two_at, of_s.outer)

    def student_outer(i, carry):
        sl[i] += times(ts_w, ts.at[i], of_s.one_at, of_s.outer) + times(ts_w, ts.at[i], of_s.two_at, of_s.outer)
        return carry

    each(student_outer)
    arrive_far(1, ws, 1)
    turn(ws, ts_w, of_s.mid_at, of_s.inner)

    def student_stats(i, carry):
        student = sl[i] + times(ts_w, ts.at[i], of_s.mid_at, of_s.inner)
        sl[i] = student
        top = jnp.max(student, axis=0, keepdims=True)
        total = jnp.sum(jnp.exp(sl[i] - top), axis=0, keepdims=True)
        stat_s[pl.ds(i, 1), :] = top + jnp.log(total)
        gap = pre[i, :, pl.ds(una, half)] - sl[i, :, pl.ds(una, half)]
        at = (i // per, pl.ds(per + i % per, 1), pl.ds(una, half))
        stat_t[at] = jnp.sum(ex[i] * gap, axis=0, keepdims=True) * stat_t[at]
        return carry

    for i in range(images):
        student_stats(i, 0)

    sends, arriving = [], {}

    def share(src, dst, k):
        for j in range(mp - 1):
            up, down = mp - 1 - j, j
            peer = jnp.where(2 * m < mp, up - (up <= m).astype(jnp.int32), down + (down >= m).astype(jnp.int32))
            slot = lax.rem(peer - m + mp, mp) - 1
            c = pltpu.make_async_remote_copy(
                src_ref=src, dst_ref=dst(slot), send_sem=ssend.at[k, j], recv_sem=srecv.at[k, slot],
                device_id={"mp": peer}, device_id_type=MESH,
            )
            c.start()
            sends.append(c)
        for d in range(mp - 1):
            arriving[k, d] = pltpu.make_async_remote_copy(
                src_ref=src, dst_ref=dst(d), send_sem=ssend.at[k, d], recv_sem=srecv.at[k, d],
                device_id={"mp": lax.rem(m + d + 1, mp)}, device_id_type=MESH,
            )

    share(stat_s, lambda d: gath_s.at[d], groups)

    row_move.wait_recv()
    scale = jnp.where(row == 0, inverse[:, half:], inverse[:, 0:half])
    for g in range(groups):
        for j in range(per):
            i = g * per + j
            smooth = pre[i, :, pl.ds(aff, half)] + nn(hal[...], srow[i]) * scale
            top = jnp.max(smooth, axis=0, keepdims=True)
            expo = jnp.exp(smooth - top)
            total = jnp.sum(expo, axis=0, keepdims=True)
            gap = smooth - sl[i, :, pl.ds(aff, half)]
            mean = jnp.sum(expo * gap, axis=0, keepdims=True) / total
            stat_t[g, pl.ds(j, 1), pl.ds(aff, half)] = top + jnp.log(total)
            stat_t[g, pl.ds(per + j, 1), pl.ds(aff, half)] = mean
        share(stat_t.at[g], lambda d, g=g: gath_t.at[d, g], g)

    def wait_shared(k):
        for d in range(mp - 1):
            arriving[k, d].wait_recv()

    wait_shared(groups)
    for g in range(groups):
        wait_shared(g)
        mine = [stat_t[g]] + [gath_t[d, g] for d in range(mp - 1)]
        logs_t = [v[0:per] for v in mine]
        means = [v[per : 2 * per] for v in mine]
        rows = slice(g * per, (g + 1) * per)
        logs_s = [stat_s[rows, :]] + [gath_s[d, rows, :] for d in range(mp - 1)]
        top_t = functools.reduce(jnp.maximum, logs_t)
        top_s = functools.reduce(jnp.maximum, logs_s)
        shares = [jnp.exp(v - top_t) for v in logs_t]
        sum_t = sum(shares)
        sum_s = sum(jnp.exp(v - top_s) for v in logs_s)
        weighted = sum(a * b for a, b in zip(shares, means))
        kl_buf[rows, :] = weighted / sum_t - top_t - jnp.log(sum_t) + top_s + jnp.log(sum_s)
    kl = kl_buf[...]
    weights = wide[...]
    total = jnp.sum(kl * weights, axis=-1, keepdims=True)
    number = jnp.sum(weights, axis=-1, keepdims=True)
    lanes = iota((images, 128), 1)
    tot[...] = jnp.where(lanes == 0, total, number)
    shares_out = []
    for k, peer in enumerate((across, below, diag)):
        c = pltpu.make_async_remote_copy(
            src_ref=tot, dst_ref=gtot.at[k], send_sem=tsend.at[k], recv_sem=trecv.at[k],
            device_id={"space": peer}, device_id_type=MESH,
        )
        c.start()
        shares_out.append(c)
    for r in range(edge):
        kl_ref[:, r, :] = kl[:, r * edge : (r + 1) * edge]
    for c in sends + [row_move, tok_move] + [c for key, c in moves.items() if key[1] != 0]:
        c.wait_send()
    for c in shares_out:
        c.wait_recv()
    everything = tot[...] + gtot[0] + gtot[1] + gtot[2]
    loss = everything[:, 0:1] / jnp.maximum(everything[:, 1:2], 1.0)
    diagonal = jnp.where(lanes == iota((images, 128), 0), loss, 0.0)
    loss_ref[...] = jnp.sum(diagonal, axis=0, keepdims=True)[:, 0:images]
    for c in shares_out:
        c.wait_send()


def middle(k):
    large = split(k // 4)
    first = large // 128 * 128
    second = -(-(k // 2 - large) // 128) * 128
    return first, second, k - k // 256 * 128


def split(rows):
    large = rows // 128 * 128
    return large if large < rows else rows - 128


def finish(kl_in, loss_in, kl_out, loss_out, sem):
    copies = [pltpu.make_async_copy(kl_in, kl_out, sem.at[0]), pltpu.make_async_copy(loss_in, loss_out, sem.at[1])]
    for c in copies:
        c.start()
    for c in copies:
        c.wait()


def fused(teacher_tokens, student_tokens, teacher_head, student_head, valid):
    images, _, edge, _, width = teacher_tokens.shape
    swidth = student_tokens.shape[-1]
    area = edge * edge
    n_edge = images * edge
    classes = teacher_head.shape[1]
    mp = lax.axis_size("mp")
    groups = 1
    anywhere = pl.BlockSpec(memory_space=pl.ANY)
    whole = pl.BlockSpec(memory_space=pltpu.VMEM)
    dma = pltpu.SemaphoreType.DMA
    kl, loss = pl.pallas_call(
        functools.partial(kernel, edge, mp),
        out_shape=(
            pltpu.VMEM((images, edge, edge), F32),
            pltpu.VMEM((1, images), F32),
        ),
        in_specs=[anywhere] * 5,
        out_specs=(whole, whole),
        scratch_shapes=[
            pltpu.VMEM((images, area, width), BF16),
            pltpu.VMEM((images, area, swidth), BF16),
            pltpu.VMEM((width, classes), BF16),
            pltpu.VMEM((swidth, classes), BF16),
            pltpu.VMEM((classes, width), BF16),
            pltpu.VMEM((classes, swidth), BF16),
            pltpu.VMEM((images, classes, area), F32),
            pltpu.VMEM((images, classes, area), F32),
            pltpu.VMEM((images, classes, area // 2), F32),
            pltpu.VMEM((classes, 2 * n_edge), F32),
            pltpu.VMEM((area, area), BF16),
            pltpu.VMEM((images, 2 * n_edge, area), BF16),
            pltpu.VMEM((images, n_edge, area // 2), BF16),
            pltpu.VMEM((2 * n_edge, n_edge), BF16),
            pltpu.VMEM((edge, area), BF16),
            pltpu.VMEM((classes, n_edge), BF16),
            pltpu.VMEM((classes, n_edge), BF16),
            pltpu.VMEM((classes, 2 * n_edge), BF16),
            pltpu.VMEM((n_edge, width), BF16),
            pltpu.VMEM((2 * n_edge, width), BF16),
            pltpu.VMEM((images, area), F32),
            pltpu.VMEM((groups, 2 * images // groups, area), F32),
            pltpu.VMEM((mp - 1, images, area), F32),
            pltpu.VMEM((mp - 1, groups, 2 * images // groups, area), F32),
            pltpu.VMEM((images, 128), F32),
            pltpu.VMEM((3, images, 128), F32),
            pltpu.VMEM((images, area), F32),
            pltpu.VMEM((images, area), F32),
            pltpu.VMEM((images, edge, edge), jnp.int32),
            dma((5,)),
            dma((12,)),
            dma((12,)),
            dma((2,)),
            dma((2,)),
            dma((groups + 1, mp - 1)),
            dma((groups + 1, mp - 1)),
            dma((3,)),
            dma((3,)),
        ],
        compiler_params=pltpu.CompilerParams(collective_id=0, has_side_effects=True),
    )(
        teacher_tokens.reshape(images, area, width),
        student_tokens.reshape(images, area, swidth),
        teacher_head,
        student_head,
        valid.reshape(images, edge, edge),
    )
    kl, loss = pl.pallas_call(
        finish,
        out_shape=(jax.ShapeDtypeStruct(kl.shape, F32), jax.ShapeDtypeStruct(loss.shape, F32)),
        in_specs=[whole, whole],
        out_specs=(anywhere, anywhere),
        scratch_shapes=[dma((2,))],
    )(pltpu.with_memory_space_constraint(kl, pltpu.VMEM), pltpu.with_memory_space_constraint(loss, pltpu.VMEM))
    return kl.reshape(images, 1, edge, edge), loss.reshape(images)


def shifted(block, axis, distance):
    devices = range(lax.axis_size(axis))
    route = [(i - distance, i) for i in devices if i - distance in devices]
    return lax.ppermute(block, axis, route)


def logit_move(values, offset):
    return shifted(values, "space", offset)


def extend(values, mover, side, column):
    left = mover(values[:, :, -1:, :], 1)
    left = jnp.where(column > 0, left, jnp.zeros_like(left))
    right = mover(values[:, :, :1, :], -1)
    right = jnp.where(column < side - 1, right, jnp.zeros_like(right))
    wide = jnp.concatenate([left, values, right], axis=2)
    upper = mover(wide[:, -1:, :, :], side)
    lower = mover(wide[:, :1, :, :], -side)
    return jnp.concatenate([upper, wide, lower], axis=1)


def body(teacher_tokens, student_tokens, teacher_head, student_head, valid):
    side = math.isqrt(lax.axis_size("space"))
    tile_index = lax.axis_index("space")
    tile_row = tile_index // side
    tile_column = tile_index % side
    teacher_tile = teacher_tokens[:, 0]
    student_tile = student_tokens[:, 0]
    images, edge = (teacher_tile.shape[0], teacher_tile.shape[1])
    classes_here = teacher_head.shape[1]
    source_flat = teacher_tile.reshape(-1, teacher_tile.shape[-1])
    student_flat = student_tile.reshape(-1, student_tile.shape[-1])
    teacher_logits = jnp.dot(
        source_flat,
        lax.all_gather(teacher_head, "space", axis=0, tiled=True),
        preferred_element_type=jnp.float32,
    )
    student_logits = jnp.dot(
        student_flat,
        lax.all_gather(student_head, "space", axis=0, tiled=True),
        preferred_element_type=jnp.float32,
    )
    teacher_wide = extend(
        teacher_logits.reshape(images, edge, edge, classes_here), logit_move, side, tile_column
    )
    extent = side * edge
    total = jnp.zeros((images, edge, edge, classes_here), jnp.float32)
    for shift_y in range(3):
        for shift_x in range(3):
            total = total + teacher_wide[:, shift_y : shift_y + edge, shift_x : shift_x + edge, :]
    places_y = tile_row * edge + jnp.arange(edge)
    places_x = tile_column * edge + jnp.arange(edge)
    line_y = 1.0 + (places_y > 0).astype(jnp.float32) + (places_y < extent - 1).astype(jnp.float32)
    line_x = 1.0 + (places_x > 0).astype(jnp.float32) + (places_x < extent - 1).astype(jnp.float32)
    counts = line_y[:, None] * line_x[None, :]
    smoothed = total / counts[None, :, :, None]
    student = student_logits.reshape(images, edge, edge, classes_here)
    top_t, top_s = lax.pmax((jnp.max(smoothed, axis=-1), jnp.max(student, axis=-1)), "mp")
    expo_t = jnp.exp(smoothed - top_t[..., None])
    sum_t, weighted, sum_s = lax.psum(
        (
            jnp.sum(expo_t, axis=-1),
            jnp.sum(expo_t * (smoothed - student), axis=-1),
            jnp.sum(jnp.exp(student - top_s[..., None]), axis=-1),
        ),
        "mp",
    )
    divergence = weighted / sum_t - top_t - jnp.log(sum_t) + top_s + jnp.log(sum_s)
    weights = valid[:, 0].astype(jnp.float32)
    totals, numbers = lax.psum(
        (jnp.sum(divergence * weights, axis=(1, 2)), jnp.sum(weights, axis=(1, 2))), "space"
    )
    image_loss = totals / jnp.maximum(numbers, 1.0)
    return (divergence[:, None], image_loss)


def fits(rows):
    if rows % 32 or rows <= 128:
        return False
    first, second, far = middle(4 * rows)
    return second > first > 0 and first == far - second


def chosen(teacher_tokens, student_tokens, teacher_head, student_head, valid):
    operands = (teacher_tokens, student_tokens, teacher_head, student_head, valid)
    aligned = (
        lax.axis_size("space") == 4
        and lax.axis_size("mp") > 1
        and teacher_tokens.shape[2] % 16 == 0
        and teacher_tokens.shape[0] % 8 == 0
        and teacher_tokens.shape[0] * teacher_tokens.shape[2] % 128 == 0
        and all(fits(head.shape[0]) for head in (teacher_head, student_head))
    )
    return fused(*operands) if aligned else body(*operands)


def solution(mesh):
    in_specs = (
        P("dp", "space", None, None, None),
        P("dp", "space", None, None, None),
        P(("dp", "space"), "mp"),
        P(("dp", "space"), "mp"),
        P("dp", "space", None, None),
    )
    out_specs = (P("dp", "space", None, None), P("dp"))
    return jax.shard_map(chosen, mesh=mesh, in_specs=in_specs, out_specs=out_specs, check_vma=False)
```

```python
import functools
import math

import jax
import jax.numpy as jnp
from jax import lax
from jax.experimental import pallas as pl
from jax.experimental.pallas import tpu as pltpu
from jax.sharding import PartitionSpec as P

MESH = pl.DeviceIdType.MESH
F32 = jnp.float32
BF16 = jnp.bfloat16


def kernel(
    edge, mp,
    tt_hbm, ts_hbm, wt_hbm, ws_hbm, valid_hbm,
    kl_ref, loss_ref,
    tt, ts, wt, ws, tt_w, ts_w, pre, sl, ex, ec, smat, scol, srow, slift, spick, hal, row_out, col_hl, tok_out, tok_x,
    stat_s, stat_t, gath_s, gath_t, tot, gtot, wide, kl_buf,
    valid_ref,
    loc_sem, wsend, wrecv, hsend, hrecv, ssend, srecv, tsend, trecv,
):
    t = lax.axis_index("space")
    m = lax.axis_index("mp")
    row, col = t // 2, t % 2
    across = 1 - col + 2 * row
    below = col + 2 * (1 - row)
    diag = 3 - t
    images = tt.shape[0]
    area = edge * edge
    groups = stat_t.shape[0]
    per = images // groups
    n_edge = images * edge

    barrier = pltpu.get_barrier_semaphore()
    for peer in (across, below, diag):
        pl.semaphore_signal(barrier, inc=1, device_id={"space": peer}, device_id_type=MESH)
    for d in range(1, mp):
        pl.semaphore_signal(barrier, inc=1, device_id={"mp": lax.rem(m + d, mp)}, device_id_type=MESH)

    local = []
    for k, (src, w) in enumerate(((wt_hbm, wt), (ws_hbm, ws))):
        n = src.shape[0]
        dst = w.at[pl.ds(pl.multiple_of(t * n, 16), n)]
        local.append(pltpu.make_async_copy(src, dst, loc_sem.at[k]))
    local.append(pltpu.make_async_copy(tt_hbm, tt, loc_sem.at[2]))
    local.append(pltpu.make_async_copy(ts_hbm, ts, loc_sem.at[3]))
    local.append(pltpu.make_async_copy(valid_hbm, valid_ref, loc_sem.at[4]))
    for c in local:
        c.start()

    local[0].wait()
    pl.semaphore_wait(barrier, 3 + mp - 1)

    def piece(w, owner, chunk):
        n = w.shape[0] // 4
        large = split(n)
        side = lax.rem(owner, 2)
        if chunk == 0:
            start, size = owner * n + side * (n - large), large
        else:
            start, size = owner * n + (1 - side) * large, n - large
        return w.at[pl.ds(pl.multiple_of(start, 16), size)]

    def move(w, k, kind, owner, chunk, peer):
        i = (k * 3 + kind) * 2 + chunk
        ref = piece(w, owner, chunk)
        return pltpu.make_async_remote_copy(
            src_ref=ref, dst_ref=ref, send_sem=wsend.at[i], recv_sem=wrecv.at[i],
            device_id={"space": peer}, device_id_type=MESH,
        )

    moves = {}
    for k, w in enumerate((wt, ws)):
        for chunk in range(2):
            moves[k, 0, chunk] = move(w, k, 0, t, chunk, below)
            moves[k, 1, chunk] = move(w, k, 1, t, chunk, across)
            moves[k, 2, chunk] = move(w, k, 2, below, chunk, across)
    for k in range(2):
        if k == 1:
            local[1].wait()
        for chunk in range(2):
            if k == 0:
                moves[k, 0, chunk].start()
            moves[k, 1, chunk].start()

    e_y = (edge - 1) * (1 - row)
    e_x = (edge - 1) * (1 - col)

    def one_hot(where):
        return jnp.where(where, 1.0, 0.0).astype(BF16)

    def iota(shape, axis):
        return lax.broadcasted_iota(jnp.int32, shape, axis)

    half = area // 2
    una, aff = pl.multiple_of(row * half, 128), pl.multiple_of((1 - row) * half, 128)
    q, p = iota((area, area), 0), iota((area, area), 1)
    smat[...] = one_hot((jnp.abs(p // edge - q // edge) <= 1) & (jnp.abs(p % edge - q % edge) <= 1))
    h, p = iota((n_edge, area), 0), iota((n_edge, area), 1)
    from_col = (p % edge == e_x) & (jnp.abs(p // edge - h % edge) <= 1)
    h2, p2 = iota((n_edge, half), 0), iota((n_edge, half), 1) + aff
    from_row = (p2 // edge == e_y) & (p2 % edge == h2 % edge)
    for i in range(images):
        scol[i, 0:n_edge, :] = one_hot(from_col & (h // edge == i))
        scol[i, n_edge:, :] = scol[i, 0:n_edge, :]
        srow[i] = one_hot(from_row & (h2 // edge == i))
    a, b = iota((n_edge, n_edge), 0), iota((n_edge, n_edge), 1)
    slift[0:n_edge, :] = one_hot((a // edge == b // edge) & (jnp.abs(a - b) <= 1))
    slift[n_edge:, :] = one_hot((a == b // edge * edge + e_y) & (b % edge == e_x))
    a, b = iota((edge, area), 0), iota((edge, area), 1)
    spick[...] = one_hot(b == a * edge + e_x)
    p = iota((1, area), 1)
    last = 2 * edge - 1
    g_y, g_x = p // edge + row * edge, p % edge + col * edge
    line_y = 1.0 + jnp.where(g_y > 0, 1.0, 0.0) + jnp.where(g_y < last, 1.0, 0.0)
    line_x = 1.0 + jnp.where(g_x > 0, 1.0, 0.0) + jnp.where(g_x < last, 1.0, 0.0)
    inverse = 1.0 / (line_y * line_x)

    def nn(x, y):
        return jnp.dot(x, y, preferred_element_type=F32)

    local[2].wait()
    for i in range(images):
        tok_out[i * edge : (i + 1) * edge, :] = nn(spick[...], tt[i]).astype(BF16)
    tok_move = pltpu.make_async_remote_copy(
        src_ref=tok_out, dst_ref=tok_x.at[pl.ds(n_edge, n_edge)], send_sem=hsend.at[1], recv_sem=hrecv.at[1],
        device_id={"space": across}, device_id_type=MESH,
    )
    tok_move.start()
    tok_x[0:n_edge, :] = tt[:, pl.ds(pl.multiple_of(e_y * edge, 16), edge), :].reshape(n_edge, tt.shape[-1])

    local[4].wait()
    for r in range(edge):
        wide[:, r * edge : (r + 1) * edge] = valid_ref[:, r, :].astype(F32)

    def turn(w, w_t, start, size):
        for j in range(0, size, 128):
            at = pl.multiple_of(start + j, 128)
            w_t[:, pl.ds(at, 128)] = w[pl.ds(at, 128), :].T

    def times(w_t, tokens, start, size):
        at = pl.ds(pl.multiple_of(start, 128), size)
        return lax.dot_general(
            w_t[:, at], tokens[:, at], (((1,), (1,)), ((), ())), preferred_element_type=F32
        )

    def own(k, w):
        for chunk in range(2):
            move(w, k, 1, across, chunk, across).wait_recv()

    def arrive(k, w, chunk):
        move(w, k, 0, below, chunk, below).wait_recv()
        moves[k, 2, chunk].start()

    def arrive_far(k, w, chunk):
        move(w, k, 2, diag, chunk, across).wait_recv()

    def each(f):
        lax.fori_loop(0, images, f, 0, unroll=images)

    class Parts:
        def __init__(self, k):
            large = split(k // 4)
            near = k // 256 * 128
            first, second, far = middle(k)
            self.near = near
            self.outer, self.inner = first, second - first
            self.near_at = row * (k - near)
            self.one_at = (1 - row) * (k - far)
            self.two_at = row * second + (1 - row) * (k - first)
            self.mid_at = row * first + (1 - row) * (k - second)

    of_t, of_s = Parts(tt.shape[-1]), Parts(ts.shape[-1])
    own(0, wt)
    turn(wt, tt_w, of_t.near_at, of_t.near)

    def teacher_near(i, carry):
        pre[i] = times(tt_w, tt.at[i], of_t.near_at, of_t.near)
        return carry

    each(teacher_near)
    own(1, ws)
    turn(ws, ts_w, of_s.near_at, of_s.near)
    local[3].wait()

    def student_near(i, carry):
        sl[i] = times(ts_w, ts.at[i], of_s.near_at, of_s.near)
        return carry

    each(student_near)
    for chunk in range(2):
        moves[0, 0, chunk].wait_send()
    for chunk in range(2):
        moves[1, 0, chunk].start()
    tok_move.wait_recv()
    ec[...] = times(tt_w, tok_x, of_t.near_at, of_t.near)

    arrive(0, wt, 0)
    arrive(0, wt, 1)
    arrive_far(0, wt, 0)
    turn(wt, tt_w, of_t.one_at, of_t.outer)
    turn(wt, tt_w, of_t.two_at, of_t.outer)
    ec[...] += times(tt_w, tok_x, of_t.one_at, of_t.outer) + times(tt_w, tok_x, of_t.two_at, of_t.outer)

    def teacher_outer(i, carry):
        pre[i] += times(tt_w, tt.at[i], of_t.one_at, of_t.outer) + times(tt_w, tt.at[i], of_t.two_at, of_t.outer)
        return carry

    each(teacher_outer)
    arrive_far(0, wt, 1)
    turn(wt, tt_w, of_t.mid_at, of_t.inner)

    def two(x):
        top = x.astype(BF16)
        return top, (x - top.astype(F32)).astype(BF16)

    e_hi, e_lo = two(ec[...] + times(tt_w, tok_x, of_t.mid_at, of_t.inner))
    row_out[...] = (nn(e_hi, slift[...]) + nn(e_lo, slift[...])).astype(BF16)
    row_move = pltpu.make_async_remote_copy(
        src_ref=row_out, dst_ref=hal, send_sem=hsend.at[0], recv_sem=hrecv.at[0],
        device_id={"space": below}, device_id_type=MESH,
    )
    col_hl[:, 0:n_edge] = e_hi[:, n_edge:]
    col_hl[:, n_edge:] = e_lo[:, n_edge:]

    def teacher_inner(i, carry):
        top, rest = two(pre[i] + times(tt_w, tt.at[i], of_t.mid_at, of_t.inner))
        pre[i] = (nn(top, smat[...]) + nn(rest, smat[...]) + nn(col_hl[...], scol[i])) * inverse
        return carry

    each(teacher_inner)

    for chunk in range(2):
        moves[1, 0, chunk].wait_send()
    row_move.start()

    def teacher_half(i, carry):
        top = jnp.max(pre[i, :, pl.ds(una, half)], axis=0, keepdims=True)
        expo = jnp.exp(pre[i, :, pl.ds(una, half)] - top)
        ex[i] = expo
        total = jnp.sum(expo, axis=0, keepdims=True)
        stat_t[i // per, pl.ds(i % per, 1), pl.ds(una, half)] = top + jnp.log(total)
        stat_t[i // per, pl.ds(per + i % per, 1), pl.ds(una, half)] = 1.0 / total
        return carry

    for i in range(images):
        teacher_half(i, 0)

    arrive(1, ws, 0)
    arrive(1, ws, 1)
    arrive_far(1, ws, 0)
    turn(ws, ts_w, of_s.one_at, of_s.outer)
    turn(ws, ts_w, of_s.two_at, of_s.outer)

    arrive_far(1, ws, 1)
    turn(ws, ts_w, of_s.mid_at, of_s.inner)

    def student_stats(i, carry):
        student = sl[i] + (
            times(ts_w, ts.at[i], of_s.one_at, of_s.outer)
            + times(ts_w, ts.at[i], of_s.two_at, of_s.outer)
            + times(ts_w, ts.at[i], of_s.mid_at, of_s.inner)
        )
        sl[i] = student
        top = jnp.max(student, axis=0, keepdims=True)
        total = jnp.sum(jnp.exp(sl[i] - top), axis=0, keepdims=True)
        stat_s[pl.ds(i, 1), :] = top + jnp.log(total)
        gap = pre[i, :, pl.ds(una, half)] - sl[i, :, pl.ds(una, half)]
        at = (i // per, pl.ds(per + i % per, 1), pl.ds(una, half))
        stat_t[at] = jnp.sum(ex[i] * gap, axis=0, keepdims=True) * stat_t[at]
        return carry

    for i in range(images):
        student_stats(i, 0)

    sends, arriving = [], {}

    def share(src, dst, k):
        for j in range(mp - 1):
            up, down = mp - 1 - j, j
            peer = jnp.where(2 * m < mp, up - (up <= m).astype(jnp.int32), down + (down >= m).astype(jnp.int32))
            slot = lax.rem(peer - m + mp, mp) - 1
            c = pltpu.make_async_remote_copy(
                src_ref=src, dst_ref=dst(slot), send_sem=ssend.at[k, j], recv_sem=srecv.at[k, slot],
                device_id={"mp": peer}, device_id_type=MESH,
            )
            c.start()
            sends.append(c)
        for d in range(mp - 1):
            arriving[k, d] = pltpu.make_async_remote_copy(
                src_ref=src, dst_ref=dst(d), send_sem=ssend.at[k, d], recv_sem=srecv.at[k, d],
                device_id={"mp": lax.rem(m + d + 1, mp)}, device_id_type=MESH,
            )

    share(stat_s, lambda d: gath_s.at[d], groups)

    row_move.wait_recv()
    scale = jnp.where(row == 0, inverse[:, half:], inverse[:, 0:half])
    for g in range(groups):
        for j in range(per):
            i = g * per + j
            smooth = pre[i, :, pl.ds(aff, half)] + nn(hal[...], srow[i]) * scale
            top = jnp.max(smooth, axis=0, keepdims=True)
            expo = jnp.exp(smooth - top)
            total = jnp.sum(expo, axis=0, keepdims=True)
            gap = smooth - sl[i, :, pl.ds(aff, half)]
            mean = jnp.sum(expo * gap, axis=0, keepdims=True) / total
            stat_t[g, pl.ds(j, 1), pl.ds(aff, half)] = top + jnp.log(total)
            stat_t[g, pl.ds(per + j, 1), pl.ds(aff, half)] = mean
        share(stat_t.at[g], lambda d, g=g: gath_t.at[d, g], g)

    def wait_shared(k):
        for d in range(mp - 1):
            arriving[k, d].wait_recv()

    wait_shared(groups)
    for g in range(groups):
        wait_shared(g)
        mine = [stat_t[g]] + [gath_t[d, g] for d in range(mp - 1)]
        logs_t = [v[0:per] for v in mine]
        means = [v[per : 2 * per] for v in mine]
        rows = slice(g * per, (g + 1) * per)
        logs_s = [stat_s[rows, :]] + [gath_s[d, rows, :] for d in range(mp - 1)]
        top_t = functools.reduce(jnp.maximum, logs_t)
        top_s = functools.reduce(jnp.maximum, logs_s)
        shares = [jnp.exp(v - top_t) for v in logs_t]
        sum_t = sum(shares)
        sum_s = sum(jnp.exp(v - top_s) for v in logs_s)
        weighted = sum(a * b for a, b in zip(shares, means))
        kl_buf[rows, :] = weighted / sum_t - top_t - jnp.log(sum_t) + top_s + jnp.log(sum_s)
    kl = kl_buf[...]
    weights = wide[...]
    total = jnp.sum(kl * weights, axis=-1, keepdims=True)
    number = jnp.sum(weights, axis=-1, keepdims=True)
    lanes = iota((images, 128), 1)
    tot[...] = jnp.where(lanes == 0, total, number)
    shares_out = []
    for k, peer in enumerate((across, below, diag)):
        c = pltpu.make_async_remote_copy(
            src_ref=tot, dst_ref=gtot.at[k], send_sem=tsend.at[k], recv_sem=trecv.at[k],
            device_id={"space": peer}, device_id_type=MESH,
        )
        c.start()
        shares_out.append(c)
    for r in range(edge):
        kl_ref[:, r, :] = kl[:, r * edge : (r + 1) * edge]
    for c in sends + [row_move, tok_move] + [c for key, c in moves.items() if key[1] != 0]:
        c.wait_send()
    for c in shares_out:
        c.wait_recv()
    everything = tot[...] + gtot[0] + gtot[1] + gtot[2]
    loss = everything[:, 0:1] / jnp.maximum(everything[:, 1:2], 1.0)
    diagonal = jnp.where(lanes == iota((images, 128), 0), loss, 0.0)
    loss_ref[...] = jnp.sum(diagonal, axis=0, keepdims=True)[:, 0:images]
    for c in shares_out:
        c.wait_send()


def middle(k):
    large = split(k // 4)
    first = large // 128 * 128
    second = -(-(k // 2 - large) // 128) * 128
    return first, second, k - k // 256 * 128


def split(rows):
    large = rows // 128 * 128
    return large if large < rows else rows - 128


def finish(kl_in, loss_in, kl_out, loss_out, sem):
    copies = [pltpu.make_async_copy(kl_in, kl_out, sem.at[0]), pltpu.make_async_copy(loss_in, loss_out, sem.at[1])]
    for c in copies:
        c.start()
    for c in copies:
        c.wait()


def fused(teacher_tokens, student_tokens, teacher_head, student_head, valid):
    images, _, edge, _, width = teacher_tokens.shape
    swidth = student_tokens.shape[-1]
    area = edge * edge
    n_edge = images * edge
    classes = teacher_head.shape[1]
    mp = lax.axis_size("mp")
    groups = 1
    anywhere = pl.BlockSpec(memory_space=pl.ANY)
    whole = pl.BlockSpec(memory_space=pltpu.VMEM)
    dma = pltpu.SemaphoreType.DMA
    kl, loss = pl.pallas_call(
        functools.partial(kernel, edge, mp),
        out_shape=(
            pltpu.VMEM((images, edge, edge), F32),
            pltpu.VMEM((1, images), F32),
        ),
        in_specs=[anywhere] * 5,
        out_specs=(whole, whole),
        scratch_shapes=[
            pltpu.VMEM((images, area, width), BF16),
            pltpu.VMEM((images, area, swidth), BF16),
            pltpu.VMEM((width, classes), BF16),
            pltpu.VMEM((swidth, classes), BF16),
            pltpu.VMEM((classes, width), BF16),
            pltpu.VMEM((classes, swidth), BF16),
            pltpu.VMEM((images, classes, area), F32),
            pltpu.VMEM((images, classes, area), F32),
            pltpu.VMEM((images, classes, area // 2), F32),
            pltpu.VMEM((classes, 2 * n_edge), F32),
            pltpu.VMEM((area, area), BF16),
            pltpu.VMEM((images, 2 * n_edge, area), BF16),
            pltpu.VMEM((images, n_edge, area // 2), BF16),
            pltpu.VMEM((2 * n_edge, n_edge), BF16),
            pltpu.VMEM((edge, area), BF16),
            pltpu.VMEM((classes, n_edge), BF16),
            pltpu.VMEM((classes, n_edge), BF16),
            pltpu.VMEM((classes, 2 * n_edge), BF16),
            pltpu.VMEM((n_edge, width), BF16),
            pltpu.VMEM((2 * n_edge, width), BF16),
            pltpu.VMEM((images, area), F32),
            pltpu.VMEM((groups, 2 * images // groups, area), F32),
            pltpu.VMEM((mp - 1, images, area), F32),
            pltpu.VMEM((mp - 1, groups, 2 * images // groups, area), F32),
            pltpu.VMEM((images, 128), F32),
            pltpu.VMEM((3, images, 128), F32),
            pltpu.VMEM((images, area), F32),
            pltpu.VMEM((images, area), F32),
            pltpu.VMEM((images, edge, edge), jnp.int32),
            dma((5,)),
            dma((12,)),
            dma((12,)),
            dma((2,)),
            dma((2,)),
            dma((groups + 1, mp - 1)),
            dma((groups + 1, mp - 1)),
            dma((3,)),
            dma((3,)),
        ],
        compiler_params=pltpu.CompilerParams(collective_id=0, has_side_effects=True),
    )(
        teacher_tokens.reshape(images, area, width),
        student_tokens.reshape(images, area, swidth),
        teacher_head,
        student_head,
        valid.reshape(images, edge, edge),
    )
    kl, loss = pl.pallas_call(
        finish,
        out_shape=(jax.ShapeDtypeStruct(kl.shape, F32), jax.ShapeDtypeStruct(loss.shape, F32)),
        in_specs=[whole, whole],
        out_specs=(anywhere, anywhere),
        scratch_shapes=[dma((2,))],
    )(pltpu.with_memory_space_constraint(kl, pltpu.VMEM), pltpu.with_memory_space_constraint(loss, pltpu.VMEM))
    return kl.reshape(images, 1, edge, edge), loss.reshape(images)


def shifted(block, axis, distance):
    devices = range(lax.axis_size(axis))
    route = [(i - distance, i) for i in devices if i - distance in devices]
    return lax.ppermute(block, axis, route)


def logit_move(values, offset):
    return shifted(values, "space", offset)


def extend(values, mover, side, column):
    left = mover(values[:, :, -1:, :], 1)
    left = jnp.where(column > 0, left, jnp.zeros_like(left))
    right = mover(values[:, :, :1, :], -1)
    right = jnp.where(column < side - 1, right, jnp.zeros_like(right))
    wide = jnp.concatenate([left, values, right], axis=2)
    upper = mover(wide[:, -1:, :, :], side)
    lower = mover(wide[:, :1, :, :], -side)
    return jnp.concatenate([upper, wide, lower], axis=1)


def body(teacher_tokens, student_tokens, teacher_head, student_head, valid):
    side = math.isqrt(lax.axis_size("space"))
    tile_index = lax.axis_index("space")
    tile_row = tile_index // side
    tile_column = tile_index % side
    teacher_tile = teacher_tokens[:, 0]
    student_tile = student_tokens[:, 0]
    images, edge = (teacher_tile.shape[0], teacher_tile.shape[1])
    classes_here = teacher_head.shape[1]
    source_flat = teacher_tile.reshape(-1, teacher_tile.shape[-1])
    student_flat = student_tile.reshape(-1, student_tile.shape[-1])
    teacher_logits = jnp.dot(
        source_flat,
        lax.all_gather(teacher_head, "space", axis=0, tiled=True),
        preferred_element_type=jnp.float32,
    )
    student_logits = jnp.dot(
        student_flat,
        lax.all_gather(student_head, "space", axis=0, tiled=True),
        preferred_element_type=jnp.float32,
    )
    teacher_wide = extend(
        teacher_logits.reshape(images, edge, edge, classes_here), logit_move, side, tile_column
    )
    extent = side * edge
    total = jnp.zeros((images, edge, edge, classes_here), jnp.float32)
    for shift_y in range(3):
        for shift_x in range(3):
            total = total + teacher_wide[:, shift_y : shift_y + edge, shift_x : shift_x + edge, :]
    places_y = tile_row * edge + jnp.arange(edge)
    places_x = tile_column * edge + jnp.arange(edge)
    line_y = 1.0 + (places_y > 0).astype(jnp.float32) + (places_y < extent - 1).astype(jnp.float32)
    line_x = 1.0 + (places_x > 0).astype(jnp.float32) + (places_x < extent - 1).astype(jnp.float32)
    counts = line_y[:, None] * line_x[None, :]
    smoothed = total / counts[None, :, :, None]
    student = student_logits.reshape(images, edge, edge, classes_here)
    top_t, top_s = lax.pmax((jnp.max(smoothed, axis=-1), jnp.max(student, axis=-1)), "mp")
    expo_t = jnp.exp(smoothed - top_t[..., None])
    sum_t, weighted, sum_s = lax.psum(
        (
            jnp.sum(expo_t, axis=-1),
            jnp.sum(expo_t * (smoothed - student), axis=-1),
            jnp.sum(jnp.exp(student - top_s[..., None]), axis=-1),
        ),
        "mp",
    )
    divergence = weighted / sum_t - top_t - jnp.log(sum_t) + top_s + jnp.log(sum_s)
    weights = valid[:, 0].astype(jnp.float32)
    totals, numbers = lax.psum(
        (jnp.sum(divergence * weights, axis=(1, 2)), jnp.sum(weights, axis=(1, 2))), "space"
    )
    image_loss = totals / jnp.maximum(numbers, 1.0)
    return (divergence[:, None], image_loss)


def fits(rows):
    if rows % 32 or rows <= 128:
        return False
    first, second, far = middle(4 * rows)
    return second > first > 0 and first == far - second


def chosen(teacher_tokens, student_tokens, teacher_head, student_head, valid):
    operands = (teacher_tokens, student_tokens, teacher_head, student_head, valid)
    aligned = (
        lax.axis_size("space") == 4
        and lax.axis_size("mp") > 1
        and teacher_tokens.shape[2] % 16 == 0
        and teacher_tokens.shape[0] % 8 == 0
        and teacher_tokens.shape[0] * teacher_tokens.shape[2] % 128 == 0
        and all(fits(head.shape[0]) for head in (teacher_head, student_head))
    )
    return fused(*operands) if aligned else body(*operands)


def solution(mesh):
    in_specs = (
        P("dp", "space", None, None, None),
        P("dp", "space", None, None, None),
        P(("dp", "space"), "mp"),
        P(("dp", "space"), "mp"),
        P("dp", "space", None, None),
    )
    out_specs = (P("dp", "space", None, None), P("dp"))
    return jax.shard_map(chosen, mesh=mesh, in_specs=in_specs, out_specs=out_specs, check_vma=False)
```
